128 devices in a mesh: node: 8 (over x, core), local: 16 (over y, z).
Axes of the slice: x: 4, y: 4, z: 4, core: 2. Of those that a mesh axis runs over, the one named last changes fastest.
Arguments:
- tokens: bfloat16 [8192, 7168], P(('node', 'local')), may hold values from -6 to 6
- routes: int32 [8192, 2], P(('node', 'local')), may hold values from 0 to 31, as said below
- scores: float32 [8192, 2], P(('node', 'local')), may hold values from 0.1 to 1
- gate_proj: bfloat16 [128, 7168, 512], P(('node', 'local')), may hold values from -0.0625 to 0.0625
- up_proj: bfloat16 [128, 7168, 512], P(('node', 'local')), may hold values from -0.0625 to 0.0625
- down_proj: bfloat16 [128, 512, 7168], P(('node', 'local')), may hold values from -0.125 to 0.125
Outputs:
- combined: bfloat16 [8192, 7168], P(('node', 'local'))
The draws below stay inside these ranges and needn't reach their ends.
Inputs may be any that keep to these rules, and one draw needn't show every extreme that they name: `routes`: each row names 2 different experts. The rows of one device name each expert at most 5 times, and in every draw one expert is named by exactly 5 rows of every device.
All inputs are finite; a program needn't handle non-finite values.
Results may differ from the reference program's by a relative error of at most 0.0085.
Values may be sent and summed in bfloat16 or wider, within the bound.
No kernel may reach another device: no remote copies, remote signals or barrier semaphores. Data moves between devices by JAX's collectives and lax.ppermute only.
A program may use at most 192 MiB of HBM per device.

```python
import math
import jax
import jax.numpy as jnp
from jax import lax

D = 7168
FF = 2048
SHARDS = 4
TOP = 2
TOK_DEV = 64
FF_DEV = 512
EXPERTS = 32
MOST = 5
TOKENS = 8192


def draw_routes(key, part):
    blocks = TOKENS // TOK_DEV
    base_key = jax.random.fold_in(key, 11)
    key_hot, key_cycle, key_perm, key_order = jax.random.split(base_key, 4)
    hot_expert = jax.random.randint(key_hot, (), 0, EXPERTS)
    cycle_least = max(TOP, (TOK_DEV * TOP - MOST + MOST - 1) // MOST)
    cycle_length = jax.random.randint(key_cycle, (blocks,), cycle_least, EXPERTS)
    shuffles = jax.vmap(lambda one_key: jax.random.permutation(one_key, EXPERTS - 1))(jax.random.split(key_perm, blocks))
    others = shuffles + (shuffles >= hot_expert).astype(shuffles.dtype)
    token_ids = jnp.arange(TOK_DEV)[:, None]
    slot_ids = jnp.arange(TOP)[None, :]
    leading = token_ids < MOST
    other_pos = jnp.where(leading, token_ids * (TOP - 1) + slot_ids - 1, MOST * (TOP - 1) + (token_ids - MOST) * TOP + slot_ids)
    cycle_pos = jnp.mod(other_pos[None, :, :], cycle_length[:, None, None])
    chosen = jnp.take_along_axis(others, cycle_pos.reshape(blocks, -1), axis=1).reshape(blocks, TOK_DEV, TOP)
    chosen = jnp.where((leading & (slot_ids == 0))[None, :, :], hot_expert, chosen)
    token_order = jax.vmap(lambda one_key: jax.random.permutation(one_key, TOK_DEV))(jax.random.split(key_order, blocks))
    chosen = jnp.take_along_axis(chosen, token_order[:, :, None], axis=1)
    return chosen.reshape(TOKENS, TOP).astype(jnp.int32)


def shard_levels(stream_key, shape, shards, low, largest):
    factor_of, own = 1.0, jax.random.fold_in(stream_key, 6)
    for position, shards_of in shards:
        draws = jnp.exp(jax.random.uniform(jax.random.fold_in(own, position), (shards_of,), jnp.float32, low / len(shards), largest / len(shards)))
        factor_of = factor_of * jnp.repeat(draws, shape[position] // shards_of).reshape([-1 if axis == position else 1 for axis in range(len(shape))])
    return factor_of


def noise(stream_key, dims, spread, bound, pieces=(), kind=jnp.bfloat16):
    level = shard_levels(stream_key, dims, pieces, -0.22, 0.18) if pieces else 1.0
    entries = jax.random.normal(stream_key, dims, jnp.float32) * spread * level
    return jnp.minimum(jnp.maximum(entries, -bound), bound).astype(kind)


def setup_inputs(seed: int = 0) -> dict:
    splits = jax.random.split(jax.random.key(seed), 7)
    return {
        "tokens": noise(splits[0], (TOKENS, D), 1.0, 6.0, ((0, 128),)),
        "routes": draw_routes(jax.random.fold_in(splits[6], 71), 0),
        "scores": jnp.clip(jnp.exp(math.log(1.0) - 2.3025851 * jax.random.uniform(splits[2], (TOKENS, TOP), jnp.float32) ** shard_levels(splits[2], (TOKENS, TOP), ((0, 128),), -0.2, 0.2)), 0.1, 1.0),
        "gate_proj": noise(splits[3], (EXPERTS * SHARDS, D, FF_DEV), D ** -0.5, 0.0625, ((0, 128),)),
        "up_proj": noise(splits[4], (EXPERTS * SHARDS, D, FF_DEV), D ** -0.5, 0.0625, ((0, 128),)),
        "down_proj": noise(splits[5], (EXPERTS * SHARDS, FF_DEV, D), FF ** -0.5, 0.125, ((0, 128),)),
    }


SCALE = 2.827


def reference(tokens, routes, scores, gate_proj, up_proj, down_proj):
    pair_count = TOKENS * TOP
    weights = (SCALE * scores / jnp.sum(scores, axis=1, keepdims=True)).astype(jnp.bfloat16)
    flat_exp = routes.reshape(-1).astype(jnp.int32)
    sort_order = jnp.argsort(flat_exp, stable=True).astype(jnp.int32)
    labels = jnp.arange(EXPERTS, dtype=jnp.int32)
    counts = jnp.sum((flat_exp[:, None] == labels[None, :]).astype(jnp.int32), axis=0).astype(jnp.int32)
    padded = (((counts + 127) // 128) * 128).astype(jnp.int32)
    group_ends = jnp.cumsum(padded).astype(jnp.int32)
    group_starts = (group_ends - padded).astype(jnp.int32)
    sorted_starts = (jnp.cumsum(counts) - counts).astype(jnp.int32)
    sorted_exp = flat_exp[sort_order]
    rank_list = jnp.arange(pair_count, dtype=jnp.int32)
    target_pos = (group_starts[sorted_exp] + rank_list - sorted_starts[sorted_exp]).astype(jnp.int32)
    block_count = (pair_count + 127) // 128 + EXPERTS
    slot_table = jnp.full((block_count * 128,), pair_count, jnp.int32).at[target_pos].set(sort_order)
    block_first = jnp.arange(block_count, dtype=jnp.int32) * 128
    block_exp = jnp.minimum(jnp.sum((group_ends[None, :] <= block_first[:, None]).astype(jnp.int32), axis=1), EXPERTS - 1).astype(jnp.int32)
    pair_weight = jnp.concatenate([weights.reshape(-1).astype(jnp.float32), jnp.zeros((1,), jnp.float32)])
    padded_x = jnp.concatenate([tokens, jnp.zeros((1, D), jnp.bfloat16)], axis=0)

    def accumulate(running, block_num):
        row_index = lax.dynamic_slice_in_dim(slot_table, (block_num * 128).astype(jnp.int32), 128)
        token_index = (row_index // TOP).astype(jnp.int32)
        expert = block_exp[block_num]
        row_data = padded_x[token_index]
        row_weight = pair_weight[row_index]
        first_row = (expert * SHARDS).astype(jnp.int32)
        w_gate = lax.dynamic_slice_in_dim(gate_proj, first_row, SHARDS, 0).transpose(1, 0, 2).reshape(D, FF)
        w_up = lax.dynamic_slice_in_dim(up_proj, first_row, SHARDS, 0).transpose(1, 0, 2).reshape(D, FF)
        gate_act = jnp.dot(row_data, w_gate, preferred_element_type=jnp.float32)
        up_act = jnp.dot(row_data, w_up, preferred_element_type=jnp.float32)
        hidden = (jax.nn.silu(gate_act) * up_act).astype(jnp.bfloat16)
        w_down = lax.dynamic_slice_in_dim(down_proj, first_row, SHARDS, 0)
        summed = jnp.zeros((128, D), jnp.float32)
        for shard_num in range(SHARDS):
            partial_value = jnp.dot(hidden[:, shard_num * FF_DEV:(shard_num + 1) * FF_DEV], w_down[shard_num], preferred_element_type=jnp.float32).astype(jnp.bfloat16)
            summed = summed + partial_value.astype(jnp.float32)
        running = running.at[token_index].add(summed * row_weight[:, None])
        return running, None

    running = lax.scan(accumulate, jnp.zeros((TOKENS + 1, D), jnp.float32), jnp.arange(block_count, dtype=jnp.int32))[0]
    return running[:TOKENS].astype(jnp.bfloat16)
```

```python
import jax
import jax.numpy as jnp
from jax import lax
from jax.sharding import Mesh, PartitionSpec as P

SCALE = 2.827
SLOTS = 5
AXES = ("x", "core", "y", "z")
BF = jnp.bfloat16
F32 = jnp.float32


def dot(a, b):
    return jnp.dot(a, b, preferred_element_type=F32)


def per_device(tokens, routes, scores, gate_proj, up_proj, down_proj):
    count, width = tokens.shape
    parts = 8
    piece = width // parts
    experts = 32
    group = parts * SLOTS
    weights = (SCALE * scores / jnp.sum(scores, axis=1, keepdims=True)).astype(BF)
    labels = jnp.arange(experts, dtype=jnp.int32)
    hits = routes[:, :, None] == labels[None, None, :]
    member = jnp.any(hits, axis=1)
    dense = jnp.sum(jnp.where(hits, weights[:, :, None].astype(F32), 0.0), axis=1)
    earlier = (jnp.arange(count)[:, None] > jnp.arange(count)[None, :]).astype(BF)
    rank = dot(earlier, member.astype(BF))
    slot = jnp.arange(SLOTS, dtype=F32)
    pick = (member.T[:, None, :] & (rank.T[:, None, :] == slot[None, :, None])).astype(BF)
    eye = jnp.eye(parts, dtype=BF)
    pick_parts = (pick[:, None, :, None, :] * eye[None, :, None, :, None]).reshape(
        experts * group, parts * count
    )
    stacked = tokens.reshape(count, parts, piece).transpose(1, 0, 2).reshape(parts * count, piece)
    send = dot(pick_parts, stacked).astype(BF).reshape(experts, 1, group, piece)
    send = jnp.broadcast_to(send, (experts, 4, group, piece)).reshape(experts * 4, group, piece)
    came = lax.all_to_all(send, AXES, 0, 0, tiled=True)
    near = 8
    far = experts * 4 // near
    src = jnp.arange(near * group)
    place = (src // SLOTS) % parts * (near * SLOTS) + src // group * SLOTS + src % SLOTS
    unmix = (place[None, :] == jnp.arange(near * group)[:, None]).astype(BF)
    rows = jnp.einsum("ab,gbn->gan", unmix, came.reshape(far, near * group, piece),
                      preferred_element_type=F32).astype(BF)
    rows = rows.reshape(far, parts, near * SLOTS, piece).transpose(0, 2, 1, 3)
    rows = rows.reshape(far * near * SLOTS, width)
    gate = dot(rows, gate_proj[0])
    up = dot(rows, up_proj[0])
    hidden = (jax.nn.silu(gate) * up).astype(BF)
    partial = dot(hidden, down_proj[0]).astype(BF)
    back = partial.reshape(far, near * SLOTS, parts, piece).transpose(0, 2, 1, 3)
    back = jnp.einsum("ba,gbn->gan", unmix, back.reshape(far, near * group, piece),
                      preferred_element_type=F32).astype(BF)
    home = lax.all_to_all(back.reshape(experts * 4, group, piece), AXES, 0, 0, tiled=True)
    share = pick.astype(F32) * dense.T[:, None, :]
    share = jnp.broadcast_to(
        share.transpose(2, 0, 1)[None, :, :, None, None, :]
        * jnp.eye(parts, dtype=F32)[:, None, None, None, :, None],
        (parts, count, experts, 4, parts, SLOTS),
    ).reshape(parts * count, experts * 4 * group).astype(BF)
    out = dot(share, home.reshape(experts * 4 * group, piece)).astype(BF)
    return out.reshape(parts, count, piece).transpose(1, 0, 2).reshape(count, width)


def solution(mesh):
    grid = Mesh(mesh.devices.reshape(4, 2, 4, 4), AXES)
    return jax.shard_map(
        per_device,
        mesh=grid,
        in_specs=(P(AXES, None), P(AXES, None), P(AXES, None), P(AXES, None, None), P(AXES, None, None), P(AXES, None, None)),
        out_specs=P(AXES, None),
        check_vma=False,
    )
```

```python
import functools

import jax
import jax.numpy as jnp
from jax import lax
from jax.experimental import pallas as pl
from jax.experimental.pallas import tpu as pltpu
from jax.sharding import Mesh, PartitionSpec as P


SCALE = 2.827
SLOTS = 5
AXES = ("x", "core", "y", "z")
BF = jnp.bfloat16
F32 = jnp.float32
FIRST = 3072
PARTS = 8
TOK = 64
HID = 512
OFFSETS = (
    (0, 0), (1, 0), (3, 0), (0, 1), (0, 3), (1, 1), (3, 3), (1, 3),
    (3, 1), (2, 1), (1, 2), (2, 3), (3, 2), (2, 0), (0, 2), (2, 2),
)
CHIPS = len(OFFSETS)
BLOCKS = 8
CHUNK = BLOCKS * SLOTS
ROWS = CHIPS * CHUNK
QUARTER = ROWS // 4


def dot(a, b):
    return jnp.dot(a, b, preferred_element_type=F32)


def along(x, axis, step):
    return lax.ppermute(x, axis, [(i, (i + step) % 4) for i in range(4)])


def across(x, dx, dy):
    pairs = [(a * 4 + b, (a + dx) % 4 * 4 + (b + dy) % 4) for a in range(4) for b in range(4)]
    return lax.ppermute(x, ("x", "y"), pairs)


def swap(x):
    return lax.ppermute(x, "core", [(0, 1), (1, 0)])


def cost(flops, nbytes):
    return pl.CostEstimate(flops=flops, bytes_accessed=nbytes, transcendentals=0)


def select_body(pick_ref, *refs):
    tokens = jnp.concatenate([r[...] for r in refs[:BLOCKS]], axis=0)
    rows = dot(pick_ref[...], tokens)
    for d in range(CHIPS):
        refs[BLOCKS + d][...] = rows[d * CHUNK:(d + 1) * CHUNK].astype(BF)


def select(pick, blocks):
    tile = 1024
    return pl.pallas_call(
        select_body,
        grid=(FIRST // tile,),
        in_specs=[pl.BlockSpec((ROWS, BLOCKS * TOK), lambda j: (0, 0))]
        + [pl.BlockSpec((TOK, tile), lambda j: (0, j))] * BLOCKS,
        out_specs=[pl.BlockSpec((CHUNK, tile), lambda j: (0, j))] * CHIPS,
        out_shape=[jax.ShapeDtypeStruct((CHUNK, FIRST), BF)] * CHIPS,
        cost_estimate=cost(2 * ROWS * BLOCKS * TOK * FIRST, 8_000_000),
    )(pick, *blocks)


def gate_up_body(count, *refs):
    gate_w, up_w = refs[count], refs[count + 1]
    gate, up = refs[count + 2], refs[count + 3]
    rows = jnp.concatenate([r[...] for r in refs[:count]], axis=0)

    @pl.when(pl.program_id(0) == 0)
    def _():
        gate[...] = jnp.zeros_like(gate)
        up[...] = jnp.zeros_like(up)

    gate[...] += dot(rows, gate_w[...])
    up[...] += dot(rows, up_w[...])


def gate_up(blocks, gate_w, up_w):
    tile = 1024
    count = len(blocks)
    rows, width = blocks[0].shape
    skip = FIRST // tile
    return pl.pallas_call(
        functools.partial(gate_up_body, count),
        grid=(width // tile,),
        in_specs=[pl.BlockSpec((rows, tile), lambda k: (0, k))] * count
        + [pl.BlockSpec((tile, HID), lambda k: (k + skip, 0))] * 2,
        out_specs=[pl.BlockSpec((rows * count, HID), lambda k: (0, 0))] * 2,
        out_shape=[jax.ShapeDtypeStruct((rows * count, HID), F32)] * 2,
        cost_estimate=cost(4 * rows * count * width * HID, 10_000_000),
    )(*blocks, gate_w, up_w)


def hidden_body(mix_ref, *refs):
    chunks, (gate_w, up_w, ga, ua, gb, ub, out, gate, up) = refs[:CHIPS], refs[CHIPS:]
    rows = dot(mix_ref[...], jnp.concatenate([r[...] for r in chunks], axis=0)).astype(BF)
    step = pl.program_id(0)

    @pl.when(step == 0)
    def _():
        gate[...] = jnp.zeros_like(gate)
        up[...] = jnp.zeros_like(up)

    gate[...] += dot(rows, gate_w[...])
    up[...] += dot(rows, up_w[...])

    @pl.when(step == pl.num_programs(0) - 1)
    def _():
        cut = 3 * QUARTER
        g = gate[:cut] + ga[...]
        out[:cut] = (g / (1.0 + jnp.exp(-g)) * (up[:cut] + ua[...])).astype(BF)
        g = gate[cut:] + gb[...]
        out[cut:] = (g / (1.0 + jnp.exp(-g)) * (up[cut:] + ub[...])).astype(BF)


def hidden_of(mix, chunks, gate_w, up_w, part_a, part_b):
    tile = 1024
    whole = lambda *shape: pl.BlockSpec(shape, lambda k: (0, 0))
    return pl.pallas_call(
        hidden_body,
        grid=(FIRST // tile,),
        in_specs=[whole(ROWS, ROWS)]
        + [pl.BlockSpec((CHUNK, tile), lambda k: (0, k))] * CHIPS
        + [pl.BlockSpec((tile, HID), lambda k: (k, 0))] * 2
        + [whole(3 * QUARTER, HID)] * 2
        + [whole(QUARTER, HID)] * 2,
        out_specs=whole(ROWS, HID),
        out_shape=jax.ShapeDtypeStruct((ROWS, HID), BF),
        scratch_shapes=[pltpu.VMEM((ROWS, HID), F32)] * 2,
        cost_estimate=cost(2 * ROWS * FIRST * (2 * HID + ROWS), 12_000_000),
    )(mix, *chunks, gate_w, up_w, *part_a, *part_b)


def down_blocks_body(hidden_ref, w_ref, *outs):
    rows = dot(hidden_ref[...], w_ref[...]).astype(BF)
    for k, out in enumerate(outs):
        out[...] = rows[k * QUARTER:(k + 1) * QUARTER]


def down_blocks(hidden, w_down):
    tile = 1024
    width = w_down.shape[1] - FIRST
    skip = FIRST // tile
    return pl.pallas_call(
        down_blocks_body,
        grid=(width // tile,),
        in_specs=[
            pl.BlockSpec((ROWS, HID), lambda j: (0, 0)),
            pl.BlockSpec((HID, tile), lambda j: (0, j + skip)),
        ],
        out_specs=[pl.BlockSpec((QUARTER, tile), lambda j: (0, j))] * 4,
        out_shape=[jax.ShapeDtypeStruct((QUARTER, width), BF)] * 4,
        cost_estimate=cost(2 * ROWS * HID * width, 10_000_000),
    )(hidden, w_down)


def down_chunks_body(unmix_ref, hidden_ref, w_ref, *refs):
    outs, mixed = refs[:CHIPS], refs[CHIPS]

    @pl.when(pl.program_id(0) == 0)
    def _():
        mixed[...] = dot(unmix_ref[...], hidden_ref[...]).astype(BF)

    rows = dot(mixed[...], w_ref[...])
    for d, out in enumerate(outs):
        out[...] = rows[d * CHUNK:(d + 1) * CHUNK].astype(BF)


def down_chunks(unmix, hidden, w_down):
    tile = 1024
    return pl.pallas_call(
        down_chunks_body,
        grid=(FIRST // tile,),
        in_specs=[
            pl.BlockSpec((ROWS, ROWS), lambda j: (0, 0)),
            pl.BlockSpec((ROWS, HID), lambda j: (0, 0)),
            pl.BlockSpec((HID, tile), lambda j: (0, j)),
        ],
        out_specs=[pl.BlockSpec((CHUNK, tile), lambda j: (0, j))] * CHIPS,
        out_shape=[jax.ShapeDtypeStruct((CHUNK, FIRST), BF)] * CHIPS,
        scratch_shapes=[pltpu.VMEM((ROWS, HID), BF)],
        cost_estimate=cost(2 * ROWS * HID * FIRST, 8_000_000),
    )(unmix, hidden, w_down)


def combine_body(share_ref, *refs):
    chunks, (own, other) = refs[:CHIPS], refs[CHIPS:]
    rows = dot(share_ref[...], jnp.concatenate([r[...] for r in chunks], axis=0))
    half = rows.shape[0] // 2
    own[...] = rows[:half]
    other[...] = rows[half:].astype(BF)


def combine(share, chunks):
    tile = 1024
    half = share.shape[0] // 2
    return pl.pallas_call(
        combine_body,
        grid=(FIRST // tile,),
        in_specs=[pl.BlockSpec(share.shape, lambda j: (0, 0))]
        + [pl.BlockSpec((CHUNK, tile), lambda j: (0, j))] * CHIPS,
        out_specs=[pl.BlockSpec((half, tile), lambda j: (0, j))] * 2,
        out_shape=[jax.ShapeDtypeStruct((half, FIRST), F32), jax.ShapeDtypeStruct((half, FIRST), BF)],
        cost_estimate=cost(2 * ROWS * 2 * half * FIRST, 10_000_000),
    )(share, *chunks)


def ranks(member, count):
    total = member.shape[0]
    t = jnp.arange(total)
    earlier = (t[:, None] > t[None, :]) & (t[:, None] // count == t[None, :] // count)
    return dot(earlier.astype(BF), member.astype(BF))


def same(a, b):
    return functools.reduce(jnp.logical_and, [p[:, None] == q[None, :] for p, q in zip(a, b)])


def per_device(tokens, routes, scores, gate_proj, up_proj, down_proj):
    width = tokens.shape[1]
    second = width - FIRST
    piece = second // PARTS
    experts = 32
    x, core, y = (lax.axis_index(a) for a in ("x", "core", "y"))
    w_gate, w_up, w_down = gate_proj[0], up_proj[0], down_proj[0]
    weights = (SCALE * scores / jnp.sum(scores, axis=1, keepdims=True)).astype(BF)
    slot = jnp.arange(SLOTS, dtype=F32)

    info = jnp.concatenate([routes.astype(BF), weights, jnp.zeros((TOK, 124), BF)], axis=1)
    own = jnp.concatenate([tokens[:, :FIRST], info], axis=1)
    planes = [own] + [None] * 3
    for step in (1, 3, 2):
        planes[step] = along(own, "z", step)
    twins = [swap(p) for p in planes]

    hits = routes[:, :, None] == jnp.arange(experts, dtype=jnp.int32)[None, None, :]
    member = jnp.any(hits, axis=1)
    dense = jnp.sum(jnp.where(hits, weights[:, :, None].astype(F32), 0.0), axis=1)
    rank = ranks(member, TOK)
    pick = (member.T[:, None, :] & (rank.T[:, None, :] == slot[None, :, None])).astype(BF)
    eye = jnp.eye(PARTS, dtype=BF)
    pick_parts = (pick[:, None, :, None, :] * eye[None, :, None, :, None]).reshape(
        experts * PARTS * SLOTS, PARTS * TOK
    )
    stacked = tokens[:, FIRST:].reshape(TOK, PARTS, piece).transpose(1, 0, 2).reshape(PARTS * TOK, piece)
    send = dot(pick_parts, stacked).astype(BF).reshape(experts, PARTS * SLOTS, piece)
    came = lax.all_to_all(send, ("x", "core", "y"), 0, 0, tiled=True)

    offset_x = jnp.array([o[0] for o in OFFSETS], jnp.int32)
    offset_y = jnp.array([o[1] for o in OFFSETS], jnp.int32)
    flat = jnp.arange(PARTS * QUARTER)
    here = flat % QUARTER
    chip = here // (2 * SLOTS)
    target = (flat // QUARTER, (x - offset_x[chip]) % 4, (y - offset_y[chip]) % 4,
              (core + here // SLOTS) % 2, here % SLOTS)
    src = flat // (PARTS * SLOTS)
    origin = (flat // SLOTS % PARTS, src // 8, src % 4, src // 4 % 2, flat % SLOTS)
    sort = same(target, origin).astype(BF)
    unsort = same(origin, target).astype(BF)

    flat = jnp.arange(ROWS)
    placed = (flat // QUARTER, flat % QUARTER // 10, flat % 10)
    landed = (flat % CHUNK // 10, flat // CHUNK, flat % 10)
    mix = same(placed, landed).astype(BF)
    unmix = same(landed, placed).astype(BF)

    facts = jnp.concatenate([b[:, FIRST:FIRST + 4] for pair in zip(planes, twins) for b in pair], axis=0)
    facts = facts.astype(F32)
    near = (((x + offset_x) % 4 * 2 + core) * 4 + (y + offset_y) % 4).astype(F32)
    named = facts[:, :2, None] == near[None, None, :]
    wanted = jnp.any(named, axis=1)
    worth = jnp.sum(jnp.where(named, facts[:, 2:4, None], 0.0), axis=1)
    order = ranks(wanted, TOK)
    block_eye = jnp.eye(BLOCKS, dtype=bool)
    chosen = (wanted.T[:, None, :] & (order.T[:, None, :] == slot[None, :, None])).reshape(
        CHIPS, 1, SLOTS, BLOCKS, TOK
    ) & block_eye[None, :, None, :, None]
    chosen_rows = chosen.astype(BF).reshape(ROWS, BLOCKS * TOK)
    back_mask = (wanted[:, :, None] & (order[:, :, None] == slot[None, None, :])).reshape(
        BLOCKS, TOK, CHIPS, 1, SLOTS
    ) & block_eye[:, None, None, :, None]
    share = jnp.where(back_mask, worth.reshape(BLOCKS, TOK, CHIPS, 1, 1), 0.0)
    share = share.reshape(4, 2, TOK, ROWS).transpose(1, 0, 2, 3).reshape(2 * 4 * TOK, ROWS).astype(BF)

    chunks = select(chosen_rows, [b for pair in zip(planes, twins) for b in pair])

    mine = dot(sort, came.reshape(PARTS * QUARTER, piece)).astype(BF)
    mine = mine.reshape(PARTS, QUARTER, piece).transpose(1, 0, 2).reshape(QUARTER, second)
    quarters = [mine] + [None] * 3
    for step in (1, 3, 2):
        quarters[step] = along(mine, "z", step)
    arrived = [chunks[0]] + [across(c, *o) for c, o in zip(chunks[1:], OFFSETS[1:])]

    part_a = gate_up([quarters[0], quarters[1], quarters[2]], w_gate, w_up)
    part_b = gate_up([quarters[3]], w_gate, w_up)
    hidden = hidden_of(mix, arrived, w_gate, w_up, part_a, part_b)

    outs = down_blocks(hidden, w_down)
    returned = [along(outs[step], "z", 4 - step) for step in (1, 3, 2)]
    leaving = down_chunks(unmix, hidden, w_down)
    gathered = [leaving[0]] + [across(c, -dx, -dy) for c, (dx, dy) in zip(leaving[1:], OFFSETS[1:])]

    total = outs[0].astype(F32)
    for r in returned:
        total = total + r.astype(F32)
    total = total.astype(BF).reshape(QUARTER, PARTS, piece).transpose(1, 0, 2).reshape(PARTS * QUARTER, piece)
    back = dot(unsort, total).astype(BF).reshape(experts, PARTS * SLOTS, piece)
    home = lax.all_to_all(back, ("x", "core", "y"), 0, 0, tiled=True)
    portion = jnp.where(pick > 0, dense.T[:, None, :], 0.0)
    portion = (portion.transpose(2, 0, 1)[None, :, :, None, :]
               * jnp.eye(PARTS, dtype=F32)[:, None, None, :, None])
    portion = portion.reshape(PARTS * TOK, experts * PARTS * SLOTS).astype(BF)
    right = dot(portion, home.reshape(experts * PARTS * SLOTS, piece)).astype(BF)
    right = right.reshape(PARTS, TOK, piece).transpose(1, 0, 2).reshape(TOK, second)

    kept, given = combine(share, gathered)
    both = kept + swap(given).astype(F32)
    both = both.reshape(4, TOK, FIRST)
    left = both[0]
    for step in (1, 3, 2):
        left = left + along(both[step].astype(BF), "z", 4 - step).astype(F32)
    return jnp.concatenate([left.astype(BF), right], axis=1)


def solution(mesh):
    grid = Mesh(mesh.devices.reshape(4, 2, 4, 4), AXES)
    rows, blocks = P(AXES, None), P(AXES, None, None)
    return jax.shard_map(
        per_device,
        mesh=grid,
        in_specs=(rows, rows, rows, blocks, blocks, blocks),
        out_specs=rows,
        check_vma=False,
    )
```

```python
import functools

import jax
import jax.numpy as jnp
from jax import lax
from jax.experimental import pallas as pl
from jax.experimental.pallas import tpu as pltpu
from jax.sharding import Mesh, PartitionSpec as P


SCALE = 2.827
SLOTS = 5
AXES = ("x", "core", "y", "z")
PLANE = ("x", "core", "y")
BF = jnp.bfloat16
F32 = jnp.float32
TOK = 64
EXPERTS = 32
HID = 512
FIRST = 3072
SECOND = 4096
PARTS = 8
PIECE = SECOND // PARTS
SENT = EXPERTS * PARTS * SLOTS
CHIPS = 16
BLOCKS = 8
CHUNK = BLOCKS * SLOTS
ROWS = CHIPS * CHUNK
QUARTER = ROWS // 4
STRIP = QUARTER // 2
HALF = ROWS // 2
FACTS = 128
TILE = 1024
STEP = 256


def dot(a, b):
    return jnp.dot(a, b, preferred_element_type=F32)


def cost(flops, nbytes):
    return pl.CostEstimate(flops=flops, bytes_accessed=nbytes, transcendentals=0)


def whole(*shape):
    return pl.BlockSpec(shape, lambda *_: (0,) * len(shape))


def column(rows, tile=TILE, skip=0):
    return pl.BlockSpec((rows, tile), lambda j: (0, j + skip))


def each(width, step, body):
    def run(i, carry):
        body(pl.ds(pl.multiple_of(i * step, step), step))
        return carry

    lax.fori_loop(0, width // step, run, 0)


def iota(shape, axis):
    return lax.broadcasted_iota(jnp.int32, shape, axis)


def flip(rows):
    unit = (iota((TOK, TOK), 0) == iota((TOK, TOK), 1)).astype(BF)
    return lax.dot_general(unit, rows.astype(BF), (((1,), (1,)), ((), ())), preferred_element_type=F32)


def routing(routes, scores):
    expert = routes.astype(F32)
    label = iota((EXPERTS, TOK), 0).astype(F32)
    hits = [(expert[k:k + 1] == label).astype(F32) for k in range(2)]
    earlier = (iota((TOK, TOK), 0) < iota((TOK, TOK), 1)).astype(BF)
    rank = dot((hits[0] + hits[1]).astype(BF), earlier)
    slots = [jnp.sum(hits[k] * rank, axis=0, keepdims=True) for k in range(2)]
    codes = expert * SLOTS + jnp.concatenate(slots, axis=0)
    weights = (SCALE * scores / (scores[0:1] + scores[1:2])).astype(BF)
    return codes, weights


def send_body(tokens_ref, routes_ref, scores_ref, own_ref, send_ref, pick_ref):
    codes, weights = routing(routes_ref[...], scores_ref[...])
    own_ref[:, :FIRST] = tokens_ref[:, :FIRST]
    lane = iota((TOK, FACTS), 1)
    facts = jnp.zeros((TOK, FACTS), F32)
    for at, columns in ((0, flip(codes)), (2, flip(weights))):
        for k in range(2):
            facts = jnp.where(lane == at + k, columns[:, k:k + 1], facts)
    own_ref[:, FIRST:] = facts.astype(BF)
    lanes = PARTS * TOK
    spread = (iota((TOK, lanes), 1) % TOK == iota((TOK, lanes), 0)).astype(BF)
    across = dot(codes.astype(BF), spread)
    row = iota((SENT, 1), 0)
    code = (row // (PARTS * SLOTS) * SLOTS + row % SLOTS).astype(F32)
    part = row // SLOTS % PARTS
    fits = ((code == across[0:1]) | (code == across[1:2])) & (part == iota((1, lanes), 1) // TOK)
    pick_ref[...] = jnp.where(fits, 1.0, 0.0).astype(BF)
    stacked = jnp.concatenate(
        [tokens_ref[:, FIRST + i * PIECE:FIRST + (i + 1) * PIECE] for i in range(PARTS)], axis=0
    )

    def body(rows):
        send_ref[rows, :] = dot(pick_ref[rows, :], stacked).astype(BF)

    each(SENT, 320, body)


def send(tokens, routes, scores):
    return pl.pallas_call(
        send_body,
        out_shape=[
            jax.ShapeDtypeStruct((TOK, FIRST + FACTS), BF),
            jax.ShapeDtypeStruct((SENT, PIECE), BF),
        ],
        scratch_shapes=[pltpu.VMEM((SENT, PARTS * TOK), BF)],
        cost_estimate=cost(2 * SENT * PARTS * TOK * PIECE, 3_000_000),
    )(tokens, routes, scores)


def chunk_code(shape, axis):
    at = iota(shape, axis)
    chip = at // CHUNK
    expert = (chip // 4 * 2 + lax.axis_index("core")) * 4 + chip % 4
    return (expert * SLOTS + at % SLOTS).astype(F32), at % CHUNK // SLOTS


def select_body(*refs):
    tokens, facts, (out, pick) = refs[:BLOCKS], refs[BLOCKS:2 * BLOCKS], refs[2 * BLOCKS:]

    @pl.when(pl.program_id(0) == 0)
    def _():
        stacked = jnp.concatenate([r[...] for r in facts], axis=0)
        unit = (iota((8, FACTS), 0) == iota((8, FACTS), 1)).astype(BF)
        codes = lax.dot_general(unit, stacked, (((1,), (1,)), ((), ())), preferred_element_type=F32)
        code, block = chunk_code((ROWS, 1), 0)
        fits = ((code == codes[0:1]) | (code == codes[1:2])) & (block == iota((1, BLOCKS * TOK), 1) // TOK)
        pick[...] = jnp.where(fits, 1.0, 0.0).astype(BF)

    def body(cols):
        out[:, cols] = dot(pick[...], jnp.concatenate([r[:, cols] for r in tokens], axis=0)).astype(BF)

    each(TILE, STEP, body)


FACT_SPEC = pl.BlockSpec((TOK, FACTS), lambda j: (0, FIRST // FACTS))


def select(blocks):
    return pl.pallas_call(
        select_body,
        grid=(FIRST // TILE,),
        in_specs=[column(TOK)] * BLOCKS + [FACT_SPEC] * BLOCKS,
        out_specs=column(ROWS),
        out_shape=jax.ShapeDtypeStruct((ROWS, FIRST), BF),
        scratch_shapes=[pltpu.VMEM((ROWS, BLOCKS * TOK), BF)],
        cost_estimate=cost(2 * ROWS * BLOCKS * TOK * FIRST, 8_000_000),
    )(*blocks, *blocks)


def accumulate(rows, gate_w, up_w, gate, up):
    @pl.when(pl.program_id(0) == 0)
    def _():
        gate[...] = jnp.zeros_like(gate)
        up[...] = jnp.zeros_like(up)

    def body(cols):
        gate[:, cols] += dot(rows, gate_w[:, cols])
        up[:, cols] += dot(rows, up_w[:, cols])

    each(HID, STEP, body)


def gate_up_body(count, *refs):
    accumulate(jnp.concatenate([r[...] for r in refs[:count]], axis=0), *refs[count:])


def weight_tile(skip):
    return pl.BlockSpec((TILE, HID), lambda k: (k + skip, 0))


def gate_up(blocks, gate_w, up_w):
    count = len(blocks)
    high = blocks[0].shape[0]
    rows = high * count
    return pl.pallas_call(
        functools.partial(gate_up_body, count),
        grid=(SECOND // TILE,),
        in_specs=[column(high)] * count + [weight_tile(FIRST // TILE)] * 2,
        out_specs=[whole(rows, HID)] * 2,
        out_shape=[jax.ShapeDtypeStruct((rows, HID), F32)] * 2,
        cost_estimate=cost(4 * rows * SECOND * HID, 12_000_000),
    )(*blocks, gate_w, up_w)


def hidden_body(mix_ref, rows_ref, gate_w, up_w, gate_n, up_n, gate_f, up_f, out, gate, up):
    rows = [dot(mix_ref[...], rows_ref[h * HALF:(h + 1) * HALF]).astype(BF) for h in range(2)]
    accumulate(jnp.concatenate(rows, axis=0), gate_w, up_w, gate, up)

    @pl.when(pl.program_id(0) == pl.num_programs(0) - 1)
    def _():
        for k in range(4):
            for h in range(2):
                at, mixed = k * QUARTER + h * STRIP, h * HALF + k * STRIP
                place = (0, 1, None, 2)[k]
                g_ref, u_ref = (gate_f, up_f) if place is None else (gate_n, up_n)
                off = h * STRIP + (place or 0) * QUARTER
                g = gate[mixed:mixed + STRIP] + g_ref[off:off + STRIP]
                u = up[mixed:mixed + STRIP] + u_ref[off:off + STRIP]
                out[at:at + STRIP] = (g / (1.0 + jnp.exp(-g)) * u).astype(BF)


def hidden_of(mix, rows, gate_w, up_w, near, far):
    return pl.pallas_call(
        hidden_body,
        grid=(FIRST // TILE,),
        in_specs=[whole(HALF, HALF), column(ROWS)] + [weight_tile(0)] * 2
        + [whole(3 * QUARTER, HID)] * 2 + [whole(QUARTER, HID)] * 2,
        out_specs=whole(ROWS, HID),
        out_shape=jax.ShapeDtypeStruct((ROWS, HID), BF),
        scratch_shapes=[pltpu.VMEM((ROWS, HID), F32)] * 2,
        cost_estimate=cost(2 * ROWS * FIRST * (2 * HID + HALF), 12_000_000),
    )(mix, rows, gate_w, up_w, *near, *far)


SPANS = ((0, QUARTER), (QUARTER, QUARTER), (2 * QUARTER, STRIP), (2 * QUARTER + STRIP, STRIP), (3 * QUARTER, QUARTER))


def down_quarters_body(hidden_ref, w_ref, *outs):
    def body(cols):
        rows = dot(hidden_ref[...], w_ref[:, cols]).astype(BF)
        for (at, size), out in zip(SPANS, outs):
            out[:, cols] = rows[at:at + size]

    each(TILE, STEP, body)


def down_quarters(hidden, w_down):
    return pl.pallas_call(
        down_quarters_body,
        grid=(SECOND // TILE,),
        in_specs=[whole(ROWS, HID), column(HID, skip=FIRST // TILE)],
        out_specs=[column(size) for _, size in SPANS],
        out_shape=[jax.ShapeDtypeStruct((size, SECOND), BF) for _, size in SPANS],
        cost_estimate=cost(2 * ROWS * HID * SECOND, 10_000_000),
    )(hidden, w_down)


def down_chunks_body(unmix_ref, hidden_ref, w_ref, out, mixed):
    @pl.when(pl.program_id(0) == 0)
    def _():
        for h in range(2):
            strips = [hidden_ref[k * QUARTER + h * STRIP:k * QUARTER + (h + 1) * STRIP] for k in range(4)]
            mixed[h * HALF:(h + 1) * HALF] = dot(unmix_ref[...], jnp.concatenate(strips, axis=0)).astype(BF)

    def body(cols):
        out[:, cols] = dot(mixed[...], w_ref[:, cols]).astype(BF)

    each(TILE, STEP, body)


def down_chunks(unmix, hidden, w_down):
    return pl.pallas_call(
        down_chunks_body,
        grid=(FIRST // TILE,),
        in_specs=[whole(HALF, HALF), whole(ROWS, HID), column(HID)],
        out_specs=column(ROWS),
        out_shape=jax.ShapeDtypeStruct((ROWS, FIRST), BF),
        scratch_shapes=[pltpu.VMEM((ROWS, HID), BF)],
        cost_estimate=cost(2 * ROWS * HID * FIRST, 8_000_000),
    )(unmix, hidden, w_down)


def combine_body(rows_ref, *refs):
    facts, (own, other, share) = refs[:BLOCKS], refs[BLOCKS:]
    half = own.shape[0]

    @pl.when(pl.program_id(0) == 0)
    def _():
        code, block = chunk_code((1, ROWS), 1)
        for b, ref in enumerate(facts):
            fact = ref[...].astype(F32)
            value = jnp.where(fact[:, 0:1] == code, fact[:, 2:3], 0.0) + jnp.where(
                fact[:, 1:2] == code, fact[:, 3:4], 0.0
            )
            at = (b % 2 * 4 + b // 2) * TOK
            share[at:at + TOK] = jnp.where(block == b, value, 0.0).astype(BF)

    def body(cols):
        rows = dot(share[...], rows_ref[:, cols])
        own[:, cols] = rows[:half]
        other[:, cols] = rows[half:].astype(BF)

    each(TILE, STEP, body)


def combine(rows, blocks):
    half = BLOCKS * TOK // 2
    return pl.pallas_call(
        combine_body,
        grid=(FIRST // TILE,),
        in_specs=[column(ROWS)] + [FACT_SPEC] * BLOCKS,
        out_specs=[column(half)] * 2,
        out_shape=[jax.ShapeDtypeStruct((half, FIRST), F32), jax.ShapeDtypeStruct((half, FIRST), BF)],
        scratch_shapes=[pltpu.VMEM((2 * half, ROWS), BF)],
        cost_estimate=cost(4 * ROWS * half * FIRST, 10_000_000),
    )(rows, *blocks)


def finish_body(home_ref, routes_ref, scores_ref, kept, a_ref, b_ref, c_ref, out, portion):
    left = kept[...] + a_ref[...].astype(F32) + b_ref[...].astype(F32) + c_ref[...].astype(F32)
    out[:, :FIRST] = left.astype(BF)
    codes, weights = routing(routes_ref[...], scores_ref[...])
    codes, worth = flip(codes), flip(weights)
    lane = iota((1, SENT), 1)
    code = (lane // (PARTS * SLOTS) * SLOTS + lane % SLOTS).astype(F32)
    value = jnp.where(codes[:, 0:1] == code, worth[:, 0:1], 0.0) + jnp.where(
        codes[:, 1:2] == code, worth[:, 1:2], 0.0
    )
    for i in range(PARTS):
        portion[i * TOK:(i + 1) * TOK] = jnp.where(lane // SLOTS % PARTS == i, value, 0.0).astype(BF)
    rows = dot(portion[...], home_ref[...]).astype(BF)
    for i in range(PARTS):
        out[:, FIRST + i * PIECE:FIRST + (i + 1) * PIECE] = rows[i * TOK:(i + 1) * TOK]


def finish(home, routes, scores, kept, parts):
    return pl.pallas_call(
        finish_body,
        out_shape=jax.ShapeDtypeStruct((TOK, FIRST + SECOND), BF),
        scratch_shapes=[pltpu.VMEM((PARTS * TOK, SENT), BF)],
        cost_estimate=cost(2 * SENT * PARTS * TOK * PIECE, 5_000_000),
    )(home, routes, scores, kept, *parts)


def along(x, step):
    return lax.ppermute(x, "z", [(i, (i + step) % 4) for i in range(4)])


def swap(x):
    return lax.ppermute(x, "core", [(0, 1), (1, 0)])


def same(a, b):
    return functools.reduce(jnp.logical_and, [p[:, None] == q[None, :] for p, q in zip(a, b)])


def per_device(tokens, routes, scores, gate_proj, up_proj, down_proj):
    core = lax.axis_index("core")
    w_gate, w_up, w_down = gate_proj[0], up_proj[0], down_proj[0]

    own, sending = send(tokens, routes.T, scores.T)
    planes = [own] + [None] * 3
    for step in (1, 3, 2):
        planes[step] = along(own, step)
    came = lax.all_to_all(sending.reshape(EXPERTS, PARTS * SLOTS, PIECE), PLANE, 0, 0, tiled=True)
    twins = []
    for k in range(4):
        twins.append(swap(planes[k]))
    blocks = [b for pair in zip(planes, twins) for b in pair]

    flat = jnp.arange(PARTS * QUARTER)
    here = flat % QUARTER
    chip = here // (2 * SLOTS)
    target = (flat // QUARTER, chip // 4, chip % 4, (core + here // SLOTS) % 2, here % SLOTS)
    src = flat // (PARTS * SLOTS)
    origin = (flat // SLOTS % PARTS, src // 8, src % 4, src // 4 % 2, flat % SLOTS)
    sort = same(target, origin).astype(BF)
    unsort = same(origin, target).astype(BF)

    flat = jnp.arange(HALF)
    placed = (flat // STRIP, flat % STRIP // 10, flat % 10)
    landed = (flat % CHUNK // 10, flat // CHUNK, flat % 10)
    mix = same(placed, landed).astype(BF)
    unmix = same(landed, placed).astype(BF)

    leaving = select(blocks)
    arrived = lax.all_to_all(leaving.reshape(CHIPS, CHUNK, FIRST), ("x", "y"), 0, 0, tiled=True)
    mine = dot(sort, came.reshape(PARTS * QUARTER, PIECE)).astype(BF)
    mine = mine.reshape(PARTS, QUARTER, PIECE).transpose(1, 0, 2).reshape(QUARTER, SECOND)
    ahead = along(mine, 1)
    behind = along(mine, 3)
    top = along(ahead[:STRIP], 1)
    bottom = along(behind[STRIP:], 3)

    near = gate_up([mine, ahead, behind], w_gate, w_up)
    far = gate_up([top, bottom], w_gate, w_up)
    hidden = hidden_of(mix, arrived.reshape(ROWS, FIRST), w_gate, w_up, near, far)

    kept_rows, after, past_top, past_bottom, before = down_quarters(hidden, w_down)
    add_top = along(past_top, 3)
    add_bottom = along(past_bottom, 1)
    chunks = down_chunks(unmix, hidden, w_down)
    gathered = lax.all_to_all(chunks.reshape(CHIPS, CHUNK, FIRST), ("x", "y"), 0, 0, tiled=True)

    after = jnp.concatenate([(after[:STRIP].astype(F32) + add_top.astype(F32)).astype(BF), after[STRIP:]], axis=0)
    before = jnp.concatenate([before[:STRIP], (before[STRIP:].astype(F32) + add_bottom.astype(F32)).astype(BF)], axis=0)
    after = along(after, 3)
    before = along(before, 1)

    total = kept_rows.astype(F32) + after.astype(F32) + before.astype(F32)
    total = total.astype(BF).reshape(QUARTER, PARTS, PIECE).transpose(1, 0, 2)
    back = dot(unsort, total.reshape(PARTS * QUARTER, PIECE)).astype(BF)
    home = lax.all_to_all(back.reshape(EXPERTS, PARTS * SLOTS, PIECE), PLANE, 0, 0, tiled=True)

    kept, given = combine(gathered.reshape(ROWS, FIRST), blocks)
    taken = swap(given)
    both = (kept + taken.astype(F32)).reshape(4, TOK, FIRST)
    parts = []
    for step in (1, 3, 2):
        parts.append(along(both[step].astype(BF), 4 - step))
    return finish(home.reshape(SENT, PIECE), routes.T, scores.T, both[0], parts)


def solution(mesh):
    grid = Mesh(mesh.devices.reshape(4, 2, 4, 4), AXES)
    rows, blocks = P(AXES, None), P(AXES, None, None)
    return jax.shard_map(
        per_device,
        mesh=grid,
        in_specs=(rows, rows, rows, blocks, blocks, blocks),
        out_specs=rows,
        check_vma=False,
    )
```

```python
import functools

import jax
import jax.numpy as jnp
from jax import lax
from jax.experimental import pallas as pl
from jax.experimental.pallas import tpu as pltpu
from jax.sharding import Mesh, PartitionSpec as P


SCALE = 2.827
SLOTS = 5
AXES = ("x", "core", "y", "z")
PLANE = ("x", "core", "y")
BF = jnp.bfloat16
F32 = jnp.float32
TOK = 64
EXPERTS = 32
HID = 512
FIRST = 3072
SECOND = 4096
PARTS = 8
PIECE = SECOND // PARTS
SENT = EXPERTS * PARTS * SLOTS
CHIPS = 16
BLOCKS = 8
CHUNK = BLOCKS * SLOTS
ROWS = CHIPS * CHUNK
QUARTER = ROWS // 4
STRIP = QUARTER // 2
HALF = ROWS // 2
FACTS = 128
TILE = 1024
STEP = 1024


def dot(a, b):
    return jnp.dot(a, b, preferred_element_type=F32)


def cost(flops, nbytes):
    return pl.CostEstimate(flops=flops, bytes_accessed=nbytes, transcendentals=0)


def whole(*shape):
    return pl.BlockSpec(shape, lambda *_: (0,) * len(shape))


def column(rows, tile=TILE, skip=0):
    return pl.BlockSpec((rows, tile), lambda j: (0, j + skip))


def each(width, step, body):
    for at in range(0, width, step):
        body(slice(at, at + step))


def iota(shape, axis):
    return lax.broadcasted_iota(jnp.int32, shape, axis)


def flip(rows):
    unit = (iota((TOK, TOK), 0) == iota((TOK, TOK), 1)).astype(BF)
    return lax.dot_general(unit, rows.astype(BF), (((1,), (1,)), ((), ())), preferred_element_type=F32)


def routing(routes, scores):
    expert = routes.astype(F32)
    label = iota((EXPERTS, TOK), 0).astype(F32)
    hits = [(expert[k:k + 1] == label).astype(F32) for k in range(2)]
    earlier = (iota((TOK, TOK), 0) < iota((TOK, TOK), 1)).astype(BF)
    rank = dot((hits[0] + hits[1]).astype(BF), earlier)
    slots = [jnp.sum(hits[k] * rank, axis=0, keepdims=True) for k in range(2)]
    codes = expert * SLOTS + jnp.concatenate(slots, axis=0)
    weights = (SCALE * scores / (scores[0:1] + scores[1:2])).astype(BF)
    return codes, weights


def send_body(tokens_ref, routes_ref, scores_ref, own_ref, send_ref, pick_ref):
    codes, weights = routing(routes_ref[...], scores_ref[...])
    own_ref[:, :FIRST] = tokens_ref[:, :FIRST]
    lane = iota((TOK, FACTS), 1)
    facts = jnp.zeros((TOK, FACTS), F32)
    for at, columns in ((0, flip(codes)), (2, flip(weights))):
        for k in range(2):
            facts = jnp.where(lane == at + k, columns[:, k:k + 1], facts)
    own_ref[:, FIRST:] = facts.astype(BF)
    lanes = PARTS * TOK
    spread = (iota((TOK, lanes), 1) % TOK == iota((TOK, lanes), 0)).astype(BF)
    across = dot(codes.astype(BF), spread)
    row = iota((SENT, 1), 0)
    code = (row // (PARTS * SLOTS) * SLOTS + row % SLOTS).astype(F32)
    part = row // SLOTS % PARTS
    fits = ((code == across[0:1]) | (code == across[1:2])) & (part == iota((1, lanes), 1) // TOK)
    pick_ref[...] = jnp.where(fits, 1.0, 0.0).astype(BF)
    stacked = jnp.concatenate(
        [tokens_ref[:, FIRST + i * PIECE:FIRST + (i + 1) * PIECE] for i in range(PARTS)], axis=0
    )

    def body(rows):
        send_ref[rows, :] = dot(pick_ref[rows, :], stacked).astype(BF)

    each(SENT, SENT, body)


def send(tokens, routes, scores):
    return pl.pallas_call(
        send_body,
        out_shape=[
            jax.ShapeDtypeStruct((TOK, FIRST + FACTS), BF),
            jax.ShapeDtypeStruct((SENT, PIECE), BF),
        ],
        scratch_shapes=[pltpu.VMEM((SENT, PARTS * TOK), BF)],
        cost_estimate=cost(2 * SENT * PARTS * TOK * PIECE, 3_000_000),
    )(tokens, routes, scores)


def chunk_code(shape, axis):
    at = iota(shape, axis)
    chip = at // CHUNK
    expert = (chip // 4 * 2 + lax.axis_index("core")) * 4 + chip % 4
    return (expert * SLOTS + at % SLOTS).astype(F32), at % CHUNK // SLOTS


def select_body(*refs):
    tokens, facts, (out, pick) = refs[:BLOCKS], refs[BLOCKS:2 * BLOCKS], refs[2 * BLOCKS:]

    @pl.when(pl.program_id(0) == 0)
    def _():
        stacked = jnp.concatenate([r[...] for r in facts], axis=0)
        unit = (iota((8, FACTS), 0) == iota((8, FACTS), 1)).astype(BF)
        codes = lax.dot_general(unit, stacked, (((1,), (1,)), ((), ())), preferred_element_type=F32)
        code, block = chunk_code((ROWS, 1), 0)
        fits = ((code == codes[0:1]) | (code == codes[1:2])) & (block == iota((1, BLOCKS * TOK), 1) // TOK)
        pick[...] = jnp.where(fits, 1.0, 0.0).astype(BF)

    def body(cols):
        out[:, cols] = dot(pick[...], jnp.concatenate([r[:, cols] for r in tokens], axis=0)).astype(BF)

    each(TILE, STEP, body)


FACT_SPEC = pl.BlockSpec((TOK, FACTS), lambda j: (0, FIRST // FACTS))


def select(blocks):
    return pl.pallas_call(
        select_body,
        grid=(FIRST // TILE,),
        in_specs=[column(TOK)] * BLOCKS + [FACT_SPEC] * BLOCKS,
        out_specs=column(ROWS),
        out_shape=jax.ShapeDtypeStruct((ROWS, FIRST), BF),
        scratch_shapes=[pltpu.VMEM((ROWS, BLOCKS * TOK), BF)],
        cost_estimate=cost(2 * ROWS * BLOCKS * TOK * FIRST, 8_000_000),
    )(*blocks, *blocks)


def accumulate(rows, gate_w, up_w, gate, up):
    @pl.when(pl.program_id(0) == 0)
    def _():
        gate[...] = jnp.zeros_like(gate)
        up[...] = jnp.zeros_like(up)

    def body(cols):
        gate[:, cols] += dot(rows, gate_w[:, cols])
        up[:, cols] += dot(rows, up_w[:, cols])

    each(HID, HID, body)


def gate_up_body(count, *refs):
    accumulate(jnp.concatenate([r[...] for r in refs[:count]], axis=0), *refs[count:])


def weight_tile(skip):
    return pl.BlockSpec((TILE, HID), lambda k: (k + skip, 0))


def gate_up(blocks, gate_w, up_w):
    count = len(blocks)
    high = blocks[0].shape[0]
    rows = high * count
    return pl.pallas_call(
        functools.partial(gate_up_body, count),
        grid=(SECOND // TILE,),
        in_specs=[column(high)] * count + [weight_tile(FIRST // TILE)] * 2,
        out_specs=[whole(rows, HID)] * 2,
        out_shape=[jax.ShapeDtypeStruct((rows, HID), F32)] * 2,
        cost_estimate=cost(4 * rows * SECOND * HID, 12_000_000),
    )(*blocks, gate_w, up_w)


def hidden_body(mix_ref, rows_ref, gate_w, up_w, gate_o, up_o, gate_n, up_n, gate_f, up_f, out, gate, up):
    rows = [dot(mix_ref[...], rows_ref[h * HALF:(h + 1) * HALF]).astype(BF) for h in range(2)]
    accumulate(jnp.concatenate(rows, axis=0), gate_w, up_w, gate, up)

    @pl.when(pl.program_id(0) == pl.num_programs(0) - 1)
    def _():
        for k in range(4):
            for h in range(2):
                at, mixed = k * QUARTER + h * STRIP, h * HALF + k * STRIP
                g_ref, u_ref = ((gate_o, up_o), (gate_n, up_n), (gate_f, up_f), (gate_n, up_n))[k]
                off = h * STRIP + (QUARTER if k == 3 else 0)
                g = gate[mixed:mixed + STRIP] + g_ref[off:off + STRIP]
                u = up[mixed:mixed + STRIP] + u_ref[off:off + STRIP]
                out[at:at + STRIP] = (g / (1.0 + jnp.exp(-g)) * u).astype(BF)


def hidden_of(mix, rows, gate_w, up_w, alone, near, far):
    return pl.pallas_call(
        hidden_body,
        grid=(FIRST // TILE,),
        in_specs=[whole(HALF, HALF), column(ROWS)] + [weight_tile(0)] * 2
        + [whole(QUARTER, HID)] * 2 + [whole(2 * QUARTER, HID)] * 2 + [whole(QUARTER, HID)] * 2,
        out_specs=whole(ROWS, HID),
        out_shape=jax.ShapeDtypeStruct((ROWS, HID), BF),
        scratch_shapes=[pltpu.VMEM((ROWS, HID), F32)] * 2,
        cost_estimate=cost(2 * ROWS * FIRST * (2 * HID + HALF), 12_000_000),
    )(mix, rows, gate_w, up_w, *alone, *near, *far)


SPANS = ((0, QUARTER), (QUARTER, QUARTER), (2 * QUARTER, STRIP), (2 * QUARTER + STRIP, STRIP), (3 * QUARTER, QUARTER))


def down_quarters_body(hidden_ref, w_ref, *outs):
    def body(cols):
        rows = dot(hidden_ref[...], w_ref[:, cols]).astype(BF)
        for (at, size), out in zip(SPANS, outs):
            out[:, cols] = rows[at:at + size]

    each(TILE, STEP, body)


def down_quarters(hidden, w_down):
    return pl.pallas_call(
        down_quarters_body,
        grid=(SECOND // TILE,),
        in_specs=[whole(ROWS, HID), column(HID, skip=FIRST // TILE)],
        out_specs=[column(size) for _, size in SPANS],
        out_shape=[jax.ShapeDtypeStruct((size, SECOND), BF) for _, size in SPANS],
        cost_estimate=cost(2 * ROWS * HID * SECOND, 10_000_000),
    )(hidden, w_down)


def down_chunks_body(unmix_ref, hidden_ref, w_ref, out, mixed):
    @pl.when(pl.program_id(0) == 0)
    def _():
        for h in range(2):
            strips = [hidden_ref[k * QUARTER + h * STRIP:k * QUARTER + (h + 1) * STRIP] for k in range(4)]
            mixed[h * HALF:(h + 1) * HALF] = dot(unmix_ref[...], jnp.concatenate(strips, axis=0)).astype(BF)

    def body(cols):
        out[:, cols] = dot(mixed[...], w_ref[:, cols]).astype(BF)

    each(TILE, STEP, body)


def down_chunks(unmix, hidden, w_down):
    return pl.pallas_call(
        down_chunks_body,
        grid=(FIRST // TILE,),
        in_specs=[whole(HALF, HALF), whole(ROWS, HID), column(HID)],
        out_specs=column(ROWS),
        out_shape=jax.ShapeDtypeStruct((ROWS, FIRST), BF),
        scratch_shapes=[pltpu.VMEM((ROWS, HID), BF)],
        cost_estimate=cost(2 * ROWS * HID * FIRST, 8_000_000),
    )(unmix, hidden, w_down)


def combine_body(rows_ref, *refs):
    facts, (own, other, share) = refs[:BLOCKS], refs[BLOCKS:]
    half = own.shape[0]

    @pl.when(pl.program_id(0) == 0)
    def _():
        code, block = chunk_code((1, ROWS), 1)
        for b, ref in enumerate(facts):
            fact = ref[...].astype(F32)
            value = jnp.where(fact[:, 0:1] == code, fact[:, 2:3], 0.0) + jnp.where(
                fact[:, 1:2] == code, fact[:, 3:4], 0.0
            )
            at = (b % 2 * 4 + b // 2) * TOK
            share[at:at + TOK] = jnp.where(block == b, value, 0.0).astype(BF)

    def body(cols):
        rows = dot(share[...], rows_ref[:, cols])
        own[:, cols] = rows[:half]
        other[:, cols] = rows[half:].astype(BF)

    each(TILE, STEP, body)


def combine(rows, blocks):
    half = BLOCKS * TOK // 2
    return pl.pallas_call(
        combine_body,
        grid=(FIRST // TILE,),
        in_specs=[column(ROWS)] + [FACT_SPEC] * BLOCKS,
        out_specs=[column(half)] * 2,
        out_shape=[jax.ShapeDtypeStruct((half, FIRST), F32), jax.ShapeDtypeStruct((half, FIRST), BF)],
        scratch_shapes=[pltpu.VMEM((2 * half, ROWS), BF)],
        cost_estimate=cost(4 * ROWS * half * FIRST, 10_000_000),
    )(rows, *blocks)


def finish_body(home_ref, routes_ref, scores_ref, kept, a_ref, b_ref, c_ref, out, portion):
    left = kept[...] + a_ref[...].astype(F32) + b_ref[...].astype(F32) + c_ref[...].astype(F32)
    out[:, :FIRST] = left.astype(BF)
    codes, weights = routing(routes_ref[...], scores_ref[...])
    codes, worth = flip(codes), flip(weights)
    lane = iota((1, SENT), 1)
    code = (lane // (PARTS * SLOTS) * SLOTS + lane % SLOTS).astype(F32)
    value = jnp.where(codes[:, 0:1] == code, worth[:, 0:1], 0.0) + jnp.where(
        codes[:, 1:2] == code, worth[:, 1:2], 0.0
    )
    for i in range(PARTS):
        portion[i * TOK:(i + 1) * TOK] = jnp.where(lane // SLOTS % PARTS == i, value, 0.0).astype(BF)
    rows = dot(portion[...], home_ref[...]).astype(BF)
    for i in range(PARTS):
        out[:, FIRST + i * PIECE:FIRST + (i + 1) * PIECE] = rows[i * TOK:(i + 1) * TOK]


def finish(home, routes, scores, kept, parts):
    return pl.pallas_call(
        finish_body,
        out_shape=jax.ShapeDtypeStruct((TOK, FIRST + SECOND), BF),
        scratch_shapes=[pltpu.VMEM((PARTS * TOK, SENT), BF)],
        cost_estimate=cost(2 * SENT * PARTS * TOK * PIECE, 5_000_000),
    )(home, routes, scores, kept, *parts)


def along(x, step):
    return lax.ppermute(x, "z", [(i, (i + step) % 4) for i in range(4)])


def swap(x):
    return lax.ppermute(x, "core", [(0, 1), (1, 0)])


def same(a, b):
    return functools.reduce(jnp.logical_and, [p[:, None] == q[None, :] for p, q in zip(a, b)])


def per_device(tokens, routes, scores, gate_proj, up_proj, down_proj):
    core = lax.axis_index("core")
    w_gate, w_up, w_down = gate_proj[0], up_proj[0], down_proj[0]

    own, sending = send(tokens, routes.T, scores.T)
    planes = [own] + [None] * 3
    for step in (1, 3, 2):
        planes[step] = along(own, step)
    came = lax.all_to_all(sending.reshape(EXPERTS, PARTS * SLOTS, PIECE), PLANE, 0, 0, tiled=True)
    twins = []
    for k in range(4):
        twins.append(swap(planes[k]))
    blocks = [b for pair in zip(planes, twins) for b in pair]

    flat = jnp.arange(PARTS * QUARTER)
    here = flat % QUARTER
    chip = here // (2 * SLOTS)
    target = (flat // QUARTER, chip // 4, chip % 4, (core + here // SLOTS) % 2, here % SLOTS)
    src = flat // (PARTS * SLOTS)
    origin = (flat // SLOTS % PARTS, src // 8, src % 4, src // 4 % 2, flat % SLOTS)
    sort = same(target, origin).astype(BF)
    unsort = same(origin, target).astype(BF)

    flat = jnp.arange(HALF)
    placed = (flat // STRIP, flat % STRIP // 10, flat % 10)
    landed = (flat % CHUNK // 10, flat // CHUNK, flat % 10)
    mix = same(placed, landed).astype(BF)
    unmix = same(landed, placed).astype(BF)

    leaving = select(blocks)
    arrived = lax.all_to_all(leaving.reshape(CHIPS, CHUNK, FIRST), ("x", "y"), 0, 0, tiled=True)
    mine = dot(sort, came.reshape(PARTS * QUARTER, PIECE)).astype(BF)
    mine = mine.reshape(PARTS, QUARTER, PIECE).transpose(1, 0, 2).reshape(QUARTER, SECOND)
    ahead = along(mine, 1)
    behind = along(mine, 3)
    top = along(ahead[:STRIP], 1)
    bottom = along(behind[STRIP:], 3)

    alone = gate_up([mine], w_gate, w_up)
    near = gate_up([ahead, behind], w_gate, w_up)
    far = gate_up([top, bottom], w_gate, w_up)
    hidden = hidden_of(mix, arrived.reshape(ROWS, FIRST), w_gate, w_up, alone, near, far)

    kept_rows, after, past_top, past_bottom, before = down_quarters(hidden, w_down)
    add_top = along(past_top, 3)
    add_bottom = along(past_bottom, 1)
    chunks = down_chunks(unmix, hidden, w_down)
    gathered = lax.all_to_all(chunks.reshape(CHIPS, CHUNK, FIRST), ("x", "y"), 0, 0, tiled=True)

    after = jnp.concatenate([(after[:STRIP].astype(F32) + add_top.astype(F32)).astype(BF), after[STRIP:]], axis=0)
    before = jnp.concatenate([before[:STRIP], (before[STRIP:].astype(F32) + add_bottom.astype(F32)).astype(BF)], axis=0)
    after = along(after, 3)
    before = along(before, 1)

    total = kept_rows.astype(F32) + after.astype(F32) + before.astype(F32)
    total = total.astype(BF).reshape(QUARTER, PARTS, PIECE).transpose(1, 0, 2)
    back = dot(unsort, total.reshape(PARTS * QUARTER, PIECE)).astype(BF)
    home = lax.all_to_all(back.reshape(EXPERTS, PARTS * SLOTS, PIECE), PLANE, 0, 0, tiled=True)

    kept, given = combine(gathered.reshape(ROWS, FIRST), blocks)
    taken = swap(given)
    both = (kept + taken.astype(F32)).reshape(4, TOK, FIRST)
    parts = []
    for step in (1, 3, 2):
        parts.append(along(both[step].astype(BF), 4 - step))
    return finish(home.reshape(SENT, PIECE), routes.T, scores.T, both[0], parts)


def solution(mesh):
    grid = Mesh(mesh.devices.reshape(4, 2, 4, 4), AXES)
    rows, blocks = P(AXES, None), P(AXES, None, None)
    return jax.shard_map(
        per_device,
        mesh=grid,
        in_specs=(rows, rows, rows, blocks, blocks, blocks),
        out_specs=rows,
        check_vma=False,
    )
```

```python
import functools

import jax
import jax.numpy as jnp
from jax import lax
from jax.experimental import pallas as pl
from jax.experimental.pallas import tpu as pltpu
from jax.sharding import Mesh, PartitionSpec as P


SCALE = 2.827
SLOTS = 5
AXES = ("x", "core", "y", "z")
PLANE = ("x", "core", "y")
BF = jnp.bfloat16
F32 = jnp.float32
TOK = 64
EXPERTS = 32
HID = 512
FIRST = 3072
SECOND = 4096
PARTS = 8
PIECE = SECOND // PARTS
SENT = EXPERTS * PARTS * SLOTS
CHIPS = 16
BLOCKS = 8
CHUNK = BLOCKS * SLOTS
ROWS = CHIPS * CHUNK
QUARTER = ROWS // 4
STRIP = QUARTER // 2
HALF = ROWS // 2
FACTS = 128
TILE = 1024
STEP = 1024


def dot(a, b):
    return jnp.dot(a, b, preferred_element_type=F32)


def cost(flops, nbytes):
    return pl.CostEstimate(flops=flops, bytes_accessed=nbytes, transcendentals=0)


def whole(*shape):
    return pl.BlockSpec(shape, lambda *_: (0,) * len(shape))


def column(rows, tile=TILE, skip=0):
    return pl.BlockSpec((rows, tile), lambda j: (0, j + skip))


def each(width, step, body):
    for at in range(0, width, step):
        body(slice(at, at + step))


def iota(shape, axis):
    return lax.broadcasted_iota(jnp.int32, shape, axis)


def flip(rows):
    unit = (iota((TOK, TOK), 0) == iota((TOK, TOK), 1)).astype(BF)
    return lax.dot_general(unit, rows.astype(BF), (((1,), (1,)), ((), ())), preferred_element_type=F32)


def routing(routes, scores):
    expert = routes.astype(F32)
    label = iota((EXPERTS, TOK), 0).astype(F32)
    hits = [(expert[k:k + 1] == label).astype(F32) for k in range(2)]
    earlier = (iota((TOK, TOK), 0) < iota((TOK, TOK), 1)).astype(BF)
    rank = dot((hits[0] + hits[1]).astype(BF), earlier)
    slots = [jnp.sum(hits[k] * rank, axis=0, keepdims=True) for k in range(2)]
    codes = expert * SLOTS + jnp.concatenate(slots, axis=0)
    weights = (SCALE * scores / (scores[0:1] + scores[1:2])).astype(BF)
    return codes, weights


def send_body(tokens_ref, routes_ref, scores_ref, own_ref, send_ref, pick_ref):
    codes, weights = routing(routes_ref[...], scores_ref[...])
    own_ref[:, :FIRST] = tokens_ref[:, :FIRST]
    lane = iota((TOK, FACTS), 1)
    facts = jnp.zeros((TOK, FACTS), F32)
    for at, columns in ((0, flip(codes)), (2, flip(weights))):
        for k in range(2):
            facts = jnp.where(lane == at + k, columns[:, k:k + 1], facts)
    own_ref[:, FIRST:] = facts.astype(BF)
    lanes = PARTS * TOK
    spread = (iota((TOK, lanes), 1) % TOK == iota((TOK, lanes), 0)).astype(BF)
    across = dot(codes.astype(BF), spread)
    row = iota((SENT, 1), 0)
    code = (row // (PARTS * SLOTS) * SLOTS + row % SLOTS).astype(F32)
    part = row // SLOTS % PARTS
    fits = ((code == across[0:1]) | (code == across[1:2])) & (part == iota((1, lanes), 1) // TOK)
    pick_ref[...] = jnp.where(fits, 1.0, 0.0).astype(BF)
    stacked = jnp.concatenate(
        [tokens_ref[:, FIRST + i * PIECE:FIRST + (i + 1) * PIECE] for i in range(PARTS)], axis=0
    )

    def body(rows):
        send_ref[rows, :] = dot(pick_ref[rows, :], stacked).astype(BF)

    each(SENT, SENT, body)


def send(tokens, routes, scores):
    return pl.pallas_call(
        send_body,
        out_shape=[
            jax.ShapeDtypeStruct((TOK, FIRST + FACTS), BF),
            jax.ShapeDtypeStruct((SENT, PIECE), BF),
        ],
        scratch_shapes=[pltpu.VMEM((SENT, PARTS * TOK), BF)],
        cost_estimate=cost(2 * SENT * PARTS * TOK * PIECE, 3_000_000),
    )(tokens, routes, scores)


def chunk_code(shape, axis):
    at = iota(shape, axis)
    chip = at // CHUNK
    expert = (chip // 4 * 2 + lax.axis_index("core")) * 4 + chip % 4
    return (expert * SLOTS + at % SLOTS).astype(F32), at % CHUNK // SLOTS


def select_body(*refs):
    tokens, facts, (out, pick) = refs[:BLOCKS], refs[BLOCKS:2 * BLOCKS], refs[2 * BLOCKS:]

    @pl.when(pl.program_id(0) == 0)
    def _():
        stacked = jnp.concatenate([r[...] for r in facts], axis=0)
        unit = (iota((8, FACTS), 0) == iota((8, FACTS), 1)).astype(BF)
        codes = lax.dot_general(unit, stacked, (((1,), (1,)), ((), ())), preferred_element_type=F32)
        code, block = chunk_code((ROWS, 1), 0)
        fits = ((code == codes[0:1]) | (code == codes[1:2])) & (block == iota((1, BLOCKS * TOK), 1) // TOK)
        pick[...] = jnp.where(fits, 1.0, 0.0).astype(BF)

    def body(cols):
        out[:, cols] = dot(pick[...], jnp.concatenate([r[:, cols] for r in tokens], axis=0)).astype(BF)

    each(TILE, STEP, body)


FACT_SPEC = pl.BlockSpec((TOK, FACTS), lambda j: (0, FIRST // FACTS))


def select(blocks):
    return pl.pallas_call(
        select_body,
        grid=(FIRST // TILE,),
        in_specs=[column(TOK)] * BLOCKS + [FACT_SPEC] * BLOCKS,
        out_specs=column(ROWS),
        out_shape=jax.ShapeDtypeStruct((ROWS, FIRST), BF),
        scratch_shapes=[pltpu.VMEM((ROWS, BLOCKS * TOK), BF)],
        cost_estimate=cost(2 * ROWS * BLOCKS * TOK * FIRST, 8_000_000),
    )(*blocks, *blocks)


def accumulate(rows, gate_w, up_w, gate, up):
    @pl.when(pl.program_id(0) == 0)
    def _():
        gate[...] = jnp.zeros_like(gate)
        up[...] = jnp.zeros_like(up)

    def body(cols):
        gate[:, cols] += dot(rows, gate_w[:, cols])
        up[:, cols] += dot(rows, up_w[:, cols])

    each(HID, HID, body)


def gate_up_body(count, *refs):
    accumulate(jnp.concatenate([r[...] for r in refs[:count]], axis=0), *refs[count:])


def weight_tile(skip):
    return pl.BlockSpec((TILE, HID), lambda k: (k + skip, 0))


def gate_up(blocks, gate_w, up_w):
    count = len(blocks)
    high = blocks[0].shape[0]
    rows = high * count
    return pl.pallas_call(
        functools.partial(gate_up_body, count),
        grid=(SECOND // TILE,),
        in_specs=[column(high)] * count + [weight_tile(FIRST // TILE)] * 2,
        out_specs=[whole(rows, HID)] * 2,
        out_shape=[jax.ShapeDtypeStruct((rows, HID), F32)] * 2,
        cost_estimate=cost(4 * rows * SECOND * HID, 12_000_000),
    )(*blocks, gate_w, up_w)


def hidden_body(mix_ref, rows_ref, gate_w, up_w, gate_o, up_o, gate_n, up_n, gate_f, up_f, out, gate, up):
    rows = [dot(mix_ref[...], rows_ref[h * HALF:(h + 1) * HALF]).astype(BF) for h in range(2)]
    accumulate(jnp.concatenate(rows, axis=0), gate_w, up_w, gate, up)

    @pl.when(pl.program_id(0) == pl.num_programs(0) - 1)
    def _():
        for k in range(4):
            for h in range(2):
                at, mixed = k * QUARTER + h * STRIP, h * HALF + k * STRIP
                g_ref, u_ref = ((gate_o, up_o), (gate_n, up_n), (gate_f, up_f), (gate_n, up_n))[k]
                off = h * STRIP + (QUARTER if k == 3 else 0)
                g = gate[mixed:mixed + STRIP] + g_ref[off:off + STRIP]
                u = up[mixed:mixed + STRIP] + u_ref[off:off + STRIP]
                out[at:at + STRIP] = (g / (1.0 + jnp.exp(-g)) * u).astype(BF)


def hidden_of(mix, rows, gate_w, up_w, alone, near, far):
    return pl.pallas_call(
        hidden_body,
        grid=(FIRST // TILE,),
        in_specs=[whole(HALF, HALF), column(ROWS)] + [weight_tile(0)] * 2
        + [whole(QUARTER, HID)] * 2 + [whole(2 * QUARTER, HID)] * 2 + [whole(QUARTER, HID)] * 2,
        out_specs=whole(ROWS, HID),
        out_shape=jax.ShapeDtypeStruct((ROWS, HID), BF),
        scratch_shapes=[pltpu.VMEM((ROWS, HID), F32)] * 2,
        cost_estimate=cost(2 * ROWS * FIRST * (2 * HID + HALF), 12_000_000),
    )(mix, rows, gate_w, up_w, *alone, *near, *far)


NEAR_SPANS = ((0, QUARTER), (QUARTER, QUARTER), (3 * QUARTER, QUARTER))
FAR_SPANS = ((2 * QUARTER, STRIP), (2 * QUARTER + STRIP, STRIP))


def down_quarters_body(spans, hidden_ref, w_ref, *outs):
    hidden = jnp.concatenate([hidden_ref[at:at + size] for at, size in spans], axis=0)
    rows = dot(hidden, w_ref[...]).astype(BF)
    done = 0
    for (_, size), out in zip(spans, outs):
        out[...] = rows[done:done + size]
        done += size


def down_quarters(spans, hidden, w_down):
    rows = sum(size for _, size in spans)
    return pl.pallas_call(
        functools.partial(down_quarters_body, spans),
        grid=(SECOND // TILE,),
        in_specs=[whole(ROWS, HID), column(HID, skip=FIRST // TILE)],
        out_specs=[column(size) for _, size in spans],
        out_shape=[jax.ShapeDtypeStruct((size, SECOND), BF) for _, size in spans],
        cost_estimate=cost(2 * rows * HID * SECOND, 8_000_000),
    )(hidden, w_down)


def down_chunks_body(unmix_ref, hidden_ref, w_ref, out, mixed):
    @pl.when(pl.program_id(0) == 0)
    def _():
        for h in range(2):
            strips = [hidden_ref[k * QUARTER + h * STRIP:k * QUARTER + (h + 1) * STRIP] for k in range(4)]
            mixed[h * HALF:(h + 1) * HALF] = dot(unmix_ref[...], jnp.concatenate(strips, axis=0)).astype(BF)

    def body(cols):
        out[:, cols] = dot(mixed[...], w_ref[:, cols]).astype(BF)

    each(TILE, STEP, body)


def down_chunks(unmix, hidden, w_down):
    return pl.pallas_call(
        down_chunks_body,
        grid=(FIRST // TILE,),
        in_specs=[whole(HALF, HALF), whole(ROWS, HID), column(HID)],
        out_specs=column(ROWS),
        out_shape=jax.ShapeDtypeStruct((ROWS, FIRST), BF),
        scratch_shapes=[pltpu.VMEM((ROWS, HID), BF)],
        cost_estimate=cost(2 * ROWS * HID * FIRST, 8_000_000),
    )(unmix, hidden, w_down)


def combine_body(rows_ref, *refs):
    facts, (own, other, share) = refs[:BLOCKS], refs[BLOCKS:]
    half = own.shape[0]

    @pl.when(pl.program_id(0) == 0)
    def _():
        code, block = chunk_code((1, ROWS), 1)
        for b, ref in enumerate(facts):
            fact = ref[...].astype(F32)
            value = jnp.where(fact[:, 0:1] == code, fact[:, 2:3], 0.0) + jnp.where(
                fact[:, 1:2] == code, fact[:, 3:4], 0.0
            )
            at = (b % 2 * 4 + b // 2) * TOK
            share[at:at + TOK] = jnp.where(block == b, value, 0.0).astype(BF)

    def body(cols):
        rows = dot(share[...], rows_ref[:, cols])
        own[:, cols] = rows[:half]
        other[:, cols] = rows[half:].astype(BF)

    each(TILE, STEP, body)


def combine(rows, blocks):
    half = BLOCKS * TOK // 2
    return pl.pallas_call(
        combine_body,
        grid=(FIRST // TILE,),
        in_specs=[column(ROWS)] + [FACT_SPEC] * BLOCKS,
        out_specs=[column(half)] * 2,
        out_shape=[jax.ShapeDtypeStruct((half, FIRST), F32), jax.ShapeDtypeStruct((half, FIRST), BF)],
        scratch_shapes=[pltpu.VMEM((2 * half, ROWS), BF)],
        cost_estimate=cost(4 * ROWS * half * FIRST, 10_000_000),
    )(rows, *blocks)


def finish_body(home_ref, routes_ref, scores_ref, kept, a_ref, b_ref, c_ref, out, portion):
    left = kept[...] + a_ref[...].astype(F32) + b_ref[...].astype(F32) + c_ref[...].astype(F32)
    out[:, :FIRST] = left.astype(BF)
    codes, weights = routing(routes_ref[...], scores_ref[...])
    codes, worth = flip(codes), flip(weights)
    lane = iota((1, SENT), 1)
    code = (lane // (PARTS * SLOTS) * SLOTS + lane % SLOTS).astype(F32)
    value = jnp.where(codes[:, 0:1] == code, worth[:, 0:1], 0.0) + jnp.where(
        codes[:, 1:2] == code, worth[:, 1:2], 0.0
    )
    for i in range(PARTS):
        portion[i * TOK:(i + 1) * TOK] = jnp.where(lane // SLOTS % PARTS == i, value, 0.0).astype(BF)
    rows = dot(portion[...], home_ref[...]).astype(BF)
    for i in range(PARTS):
        out[:, FIRST + i * PIECE:FIRST + (i + 1) * PIECE] = rows[i * TOK:(i + 1) * TOK]


def finish(home, routes, scores, kept, parts):
    return pl.pallas_call(
        finish_body,
        out_shape=jax.ShapeDtypeStruct((TOK, FIRST + SECOND), BF),
        scratch_shapes=[pltpu.VMEM((PARTS * TOK, SENT), BF)],
        cost_estimate=cost(2 * SENT * PARTS * TOK * PIECE, 5_000_000),
    )(home, routes, scores, kept, *parts)


def along(x, step):
    return lax.ppermute(x, "z", [(i, (i + step) % 4) for i in range(4)])


def swap(x):
    return lax.ppermute(x, "core", [(0, 1), (1, 0)])


def same(a, b):
    return functools.reduce(jnp.logical_and, [p[:, None] == q[None, :] for p, q in zip(a, b)])


def per_device(tokens, routes, scores, gate_proj, up_proj, down_proj):
    core = lax.axis_index("core")
    w_gate, w_up, w_down = gate_proj[0], up_proj[0], down_proj[0]

    own, sending = send(tokens, routes.T, scores.T)
    planes = [own] + [None] * 3
    for step in (1, 3, 2):
        planes[step] = along(own, step)
    came = lax.all_to_all(sending.reshape(EXPERTS, PARTS * SLOTS, PIECE), PLANE, 0, 0, tiled=True)
    twins = []
    for k in range(4):
        twins.append(swap(planes[k]))
    blocks = [b for pair in zip(planes, twins) for b in pair]

    flat = jnp.arange(PARTS * QUARTER)
    here = flat % QUARTER
    chip = here // (2 * SLOTS)
    target = (flat // QUARTER, chip // 4, chip % 4, (core + here // SLOTS) % 2, here % SLOTS)
    src = flat // (PARTS * SLOTS)
    origin = (flat // SLOTS % PARTS, src // 8, src % 4, src // 4 % 2, flat % SLOTS)
    sort = same(target, origin).astype(BF)
    unsort = same(origin, target).astype(BF)

    flat = jnp.arange(HALF)
    placed = (flat // STRIP, flat % STRIP // 10, flat % 10)
    landed = (flat % CHUNK // 10, flat // CHUNK, flat % 10)
    mix = same(placed, landed).astype(BF)
    unmix = same(landed, placed).astype(BF)

    leaving = select(blocks)
    arrived = lax.all_to_all(leaving.reshape(CHIPS, CHUNK, FIRST), ("x", "y"), 0, 0, tiled=True)
    mine = dot(sort, came.reshape(PARTS * QUARTER, PIECE)).astype(BF)
    mine = mine.reshape(PARTS, QUARTER, PIECE).transpose(1, 0, 2).reshape(QUARTER, SECOND)
    ahead = along(mine, 1)
    behind = along(mine, 3)
    top = along(ahead[:STRIP], 1)
    bottom = along(behind[STRIP:], 3)

    alone = gate_up([mine], w_gate, w_up)
    near = gate_up([ahead, behind], w_gate, w_up)
    far = gate_up([top, bottom], w_gate, w_up)
    hidden = hidden_of(mix, arrived.reshape(ROWS, FIRST), w_gate, w_up, alone, near, far)

    past_top, past_bottom = down_quarters(FAR_SPANS, hidden, w_down)
    add_top = along(past_top, 3)
    add_bottom = along(past_bottom, 1)
    chunks = down_chunks(unmix, hidden, w_down)
    gathered = lax.all_to_all(chunks.reshape(CHIPS, CHUNK, FIRST), ("x", "y"), 0, 0, tiled=True)

    kept_rows, after, before = down_quarters(NEAR_SPANS, hidden, w_down)
    after = jnp.concatenate([(after[:STRIP].astype(F32) + add_top.astype(F32)).astype(BF), after[STRIP:]], axis=0)
    before = jnp.concatenate([before[:STRIP], (before[STRIP:].astype(F32) + add_bottom.astype(F32)).astype(BF)], axis=0)
    after = along(after, 3)
    before = along(before, 1)

    total = kept_rows.astype(F32) + after.astype(F32) + before.astype(F32)
    total = total.astype(BF).reshape(QUARTER, PARTS, PIECE).transpose(1, 0, 2)
    back = dot(unsort, total.reshape(PARTS * QUARTER, PIECE)).astype(BF)
    home = lax.all_to_all(back.reshape(EXPERTS, PARTS * SLOTS, PIECE), PLANE, 0, 0, tiled=True)

    kept, given = combine(gathered.reshape(ROWS, FIRST), blocks)
    taken = swap(given)
    both = (kept + taken.astype(F32)).reshape(4, TOK, FIRST)
    parts = []
    for step in (1, 3, 2):
        parts.append(along(both[step].astype(BF), 4 - step))
    return finish(home.reshape(SENT, PIECE), routes.T, scores.T, both[0], parts)


def solution(mesh):
    grid = Mesh(mesh.devices.reshape(4, 2, 4, 4), AXES)
    rows, blocks = P(AXES, None), P(AXES, None, None)
    return jax.shard_map(
        per_device,
        mesh=grid,
        in_specs=(rows, rows, rows, blocks, blocks, blocks),
        out_specs=rows,
        check_vma=False,
    )
```
